32 devices in a mesh: inst: 4 (over y, x), scen: 8 (over z, core).
Axes of the slice: x: 2, y: 2, z: 4, core: 2. Of those that a mesh axis runs over, the one named last changes fastest.
Arguments:
- positions: int32 [512, 16384], P(None, 'inst'), may hold values from -50 to 50
- holding_block_grid: int32 [8, 128], P(None, 'inst'), may hold values 0 or 1
- risk: float32 [16384, 8192], P('inst', 'scen'), may hold values from -64 to 64
Outputs:
- margin: float32 [512], P('inst')
- gradient: float32 [512, 16384], P('scen', 'inst')
The draws below stay inside these ranges and needn't reach their ends.
All inputs are finite; a program needn't handle non-finite values. No bound on the sum of `holding_block_grid` on one device may be relied on, other than what follows from the above.
Results may differ from the reference program's by a relative error of at most 0.0003.
Values sent between devices are 32-bit elements; how exact they have to be, the bound alone decides.
A program may use at most 64 MiB of HBM per device.

```python
import math
import jax
import jax.numpy as jnp
from jax import lax

ACC = 512
INSTRUMENT_TOTAL = 16384
ABLK = 64
IBLK = 128
SCEN = 8192


def draw_risk(key, part):
    first, second, third = jax.random.split(jax.random.fold_in(key, 17), 3)
    row_scale = jnp.exp(jax.random.uniform(second, (INSTRUMENT_TOTAL, 1), jnp.float32, jnp.log(0.3), jnp.log(3.0)))
    jitter = jnp.exp(jax.random.uniform(third, (1, SCEN), jnp.float32, jnp.log(0.9), jnp.log(1.1)))
    position = jnp.arange(SCEN, dtype=jnp.float32) / SCEN
    base = jnp.clip(jax.random.normal(first, (INSTRUMENT_TOTAL, SCEN), jnp.float32), -6.0, 6.0)
    ramp = jnp.sqrt(1.0 + 2.2 * position)
    result = 0.25 * base * row_scale * (jitter * ramp[None, :])
    return result


def with_ends(values, rng, low, high):
    dims = values.shape
    index_at = [jax.random.randint(jax.random.fold_in(rng, axis), (), 0, dims[axis]) for axis in range(len(dims))]
    values = values.at[tuple(index_at)].set(low)
    longest = dims.index(max(dims))
    index_at[longest] = (index_at[longest] + 1) % dims[longest]
    return values.at[tuple(index_at)].set(high)


def setup_inputs(seed: int = 0) -> dict:
    splits = jax.random.split(jax.random.key(seed), 4)
    return {
        "positions": with_ends(jax.random.randint(splits[0], (ACC, INSTRUMENT_TOTAL), -50, 51), jax.random.fold_in(splits[0], 1), -50, 50).astype(jnp.int32),
        "holding_block_grid": with_ends((jax.random.randint(splits[1], (ACC // ABLK, INSTRUMENT_TOTAL // IBLK), 0, 4) < 3).astype(jnp.int32), jax.random.fold_in(splits[1], 1), 0, 1),
        "risk": draw_risk(jax.random.fold_in(splits[3], 71), 0),
    }


def reference(positions, holding_block_grid, risk):
    live_mask = jnp.repeat(jnp.repeat(holding_block_grid, ABLK, axis=0), IBLK, axis=1)
    held = (positions * live_mask).astype(jnp.float32)
    profit_and_losses = jnp.dot(held, risk, precision=lax.Precision.HIGHEST, preferred_element_type=jnp.float32)
    softness_level = 8.0 * math.sqrt(INSTRUMENT_TOTAL)
    tail_logits = -profit_and_losses / softness_level
    peak = lax.optimization_barrier(jnp.max(tail_logits, axis=1))
    shifted = jnp.exp(tail_logits - peak[:, None])
    total = lax.optimization_barrier(jnp.sum(shifted, axis=1))
    margin = peak + jnp.log(total) - math.log(SCEN)
    weights = shifted / total[:, None]
    gradient = -jnp.einsum('as,is->ai', weights, risk, precision=lax.Precision.HIGHEST)
    return (margin, gradient)
```

```python
import functools
import math

import jax
import jax.numpy as jnp
from jax import lax
from jax.experimental import pallas as pl
from jax.experimental.pallas import tpu as pltpu
from jax.sharding import PartitionSpec as P

ABLK = 64
IBLK = 128
CORES = 2
LANES = 128
STAGES = 3
PIECE = 1024
STRIP = 16


def chunk_plan(rows, chips, inst_number):
    unit = max(16, 2 * inst_number)
    plan = []
    for phase in range(chips // 2):
        done = 0
        while done < rows:
            small = phase == 0 and done < 2 * unit
            take = min(unit if small else 2 * unit, rows - done)
            plan.append((chips - 1 - phase, phase, done, take))
            done += take
    return plan


def kernel(
    cfg,
    positions,
    grid,
    risk,
    margin_out,
    gradient_out,
    stage,
    pos_buf,
    held,
    high,
    low,
    part,
    rs_buf,
    full,
    tails,
    peaks,
    totals,
    stats,
    factor,
    partial,
    pair_buf,
    line_buf,
    marg,
    stage_sem,
    pos_sem,
    rs_send,
    rs_recv,
    ag_send,
    ag_recv,
    stats_send,
    stats_recv,
    pair_send,
    pair_recv,
    line_send,
    line_recv,
):
    plan, accounts, insts, scens, softness, total_scen = cfg
    instruments, scen_here = risk.shape
    rows = accounts // scens
    chips = scens // CORES
    piece = min(PIECE, instruments)
    pieces = instruments // piece
    kblock = stage.shape[1]
    kblocks = instruments // kblock
    number = len(plan)
    inst = lax.axis_index("inst")
    me = lax.axis_index("scen")
    z = me // CORES
    core = me % CORES
    far = z // (chips // 2)

    sizes = [4 * take for _, _, _, take in plan]
    starts = [sum(sizes[:c]) for c in range(number)]
    head = sizes[0] + sizes[1]

    def owner_of(c, slot):
        above, below, _, _ = plan[c]
        return above - slot * (above - below)

    def load_risk(b):
        slot = b % STAGES
        return pltpu.make_async_copy(
            risk.at[pl.ds(b * kblock, kblock), :], stage.at[slot], stage_sem.at[slot]
        )

    def pos_copies(c, slot, base):
        _, _, first, take = plan[c]
        copies = []
        for s in range(2):
            for k in range(CORES):
                account = (owner_of(c, s) * CORES + k) * rows + first
                group = s * CORES + k
                copies.append(
                    pltpu.make_async_copy(
                        positions.at[pl.ds(account, take), :],
                        pos_buf.at[slot, pl.ds(base + group * take, take), :],
                        pos_sem.at[slot, base // sizes[0] if base else 0, group],
                    )
                )
        return copies

    def make_held(c, slot, base):
        _, _, first, take = plan[c]

        def column(j, carry):
            cols = pl.ds(pl.multiple_of(j * IBLK, IBLK), IBLK)
            for s in range(2):
                for k in range(CORES):
                    account = (owner_of(c, s) * CORES + k) * rows + first
                    live = grid[account // ABLK, j].astype(jnp.float32)
                    lines = pl.ds(base + (s * CORES + k) * take, take)
                    held[lines, cols] = (
                        pos_buf[slot, lines, cols].astype(jnp.float32) * live
                    ).astype(jnp.bfloat16)
            return carry

        lax.fori_loop(0, instruments // IBLK, column, 0)

    for copy in pos_copies(0, 0, 0) + pos_copies(1, 0, sizes[0]):
        copy.start()
    for b in range(min(STAGES, kblocks)):
        load_risk(b).start()
    if number > 2:
        for copy in pos_copies(2, 1, 0):
            copy.start()

    barrier = pltpu.get_barrier_semaphore()
    for i in range(1, insts):
        pl.semaphore_signal(barrier, inc=1, device_id={"inst": (inst + i) % insts})
    for i in range(1, scens):
        pl.semaphore_signal(barrier, inc=1, device_id={"scen": (me + i) % scens})

    peaks[...] = jnp.zeros_like(peaks)
    totals[...] = jnp.ones_like(totals)
    marg[...] = jnp.zeros_like(marg)
    part[pl.ds(0, head), :] = jnp.zeros((head, scen_here), jnp.float32)

    for copy in pos_copies(0, 0, 0) + pos_copies(1, 0, sizes[0]):
        copy.wait()
    make_held(0, 0, 0)
    make_held(1, 0, sizes[0])
    if number > 3:
        for copy in pos_copies(3, 0, 0):
            copy.start()

    def arrive(b, carry):
        slot = b % STAGES
        load_risk(b).wait()

        def split(r, inner):
            lines = pl.ds(pl.multiple_of(r * STRIP, STRIP), STRIP)
            value = stage[slot, lines, :]
            top = value.astype(jnp.bfloat16)
            there = pl.ds(pl.multiple_of(b * kblock + r * STRIP, STRIP), STRIP)
            high[there, :] = top
            low[there, :] = (value - top.astype(jnp.float32)).astype(jnp.bfloat16)
            return inner

        lax.fori_loop(0, kblock // STRIP, split, 0, unroll=2)

        @pl.when(b + STAGES < kblocks)
        def _():
            load_risk(b + STAGES).start()

        deep = pl.ds(pl.multiple_of(b * kblock, kblock), kblock)
        mine = held[pl.ds(0, head), deep]
        part[pl.ds(0, head), :] += jnp.dot(
            mine, high[deep, :], preferred_element_type=jnp.float32
        ) + jnp.dot(mine, low[deep, :], preferred_element_type=jnp.float32)
        return carry

    lax.fori_loop(0, kblocks, arrive, 0)

    def profit(c):
        slot = (c - 1) % 2
        for copy in pos_copies(c, slot, 0):
            copy.wait()
        make_held(c, slot, 0)
        if c + 2 < number:
            for copy in pos_copies(c + 2, slot, 0):
                copy.start()
        width = 256

        def column(n, carry):
            cols = pl.ds(pl.multiple_of(n * width, width), width)
            mine = held[pl.ds(0, sizes[c]), :]
            part[pl.ds(starts[c], sizes[c]), cols] = jnp.dot(
                mine, high[:, cols], preferred_element_type=jnp.float32
            ) + jnp.dot(mine, low[:, cols], preferred_element_type=jnp.float32)
            return carry

        lax.fori_loop(0, scen_here // width, column, 0)

    def rs_copy(c, i):
        group = sizes[c] // insts
        to = (inst + i) % insts
        return pltpu.make_async_remote_copy(
            part.at[pl.ds(pl.multiple_of(starts[c] + to * group, 8), group), :],
            rs_buf.at[i - 1, pl.ds(starts[c] // insts, group), :],
            rs_send.at[c, i - 1],
            rs_recv.at[c, i - 1],
            device_id={"inst": to},
        )

    def ag_copy(c, i, source):
        group = sizes[c] // insts
        lines = pl.ds(pl.multiple_of(starts[c] + source * group, 8), group)
        return pltpu.make_async_remote_copy(
            full.at[lines, :],
            full.at[lines, :],
            ag_send.at[c, i - 1],
            ag_recv.at[c, i - 1],
            device_id={"inst": (inst + i) % insts},
        )

    def send_parts(c):
        for i in range(1, insts):
            rs_copy(c, i).start()

    def sum_and_gather(c):
        group = sizes[c] // insts
        lines = pl.ds(pl.multiple_of(starts[c] + inst * group, 8), group)
        value = part[lines, :]
        for i in range(1, insts):
            rs_copy(c, i).wait_recv()
            value = value + rs_buf[i - 1, pl.ds(starts[c] // insts, group), :]
        full[lines, :] = value
        for i in range(1, insts):
            ag_copy(c, i, inst).start()

    def stats_copy(c, i):
        return pltpu.make_async_remote_copy(
            stats.at[c, 0],
            stats.at[c, i],
            stats_send.at[c, i - 1],
            stats_recv.at[c, i - 1],
            device_id={"scen": (me + i) % scens},
        )

    def weigh(c):
        size = sizes[c]
        for i in range(1, insts):
            ag_copy(c, i, (inst + insts - i) % insts).wait_recv()

        def strip(r, carry):
            lines = pl.ds(pl.multiple_of(r * STRIP, STRIP), STRIP)
            score = full[pl.ds(pl.multiple_of(starts[c] + r * STRIP, STRIP), STRIP), :] * (
                -1.0 / softness
            )
            peak = jnp.max(score, axis=1, keepdims=True)
            tail = jnp.exp(score - peak)
            total = jnp.sum(tail, axis=1, keepdims=True)
            top = tail.astype(jnp.bfloat16)
            tails[lines, :] = top
            tails[pl.ds(pl.multiple_of(size + r * STRIP, STRIP), STRIP), :] = (
                tail - top.astype(jnp.float32)
            ).astype(jnp.bfloat16)
            peaks[lines, :] = jnp.broadcast_to(peak, (STRIP, LANES))
            totals[lines, :] = jnp.broadcast_to(total, (STRIP, LANES))
            return carry

        lax.fori_loop(0, size // STRIP, strip, 0)
        stats[c, 0, 0:1, :] = jnp.transpose(peaks[...])[0:1, :]
        stats[c, 0, 1:2, :] = jnp.transpose(totals[...])[0:1, :]
        for i in range(1, scens):
            stats_copy(c, i).start()

    def multiply(c):
        size = sizes[c]
        width = 512
        over = (((1,), (1,)), ((), ()))

        def column(n, carry):
            cols = pl.ds(pl.multiple_of(n * width, width), width)
            both = lax.dot_general(
                tails[pl.ds(0, 2 * size), :], high[cols, :], over,
                preferred_element_type=jnp.float32,
            )
            rest = lax.dot_general(
                tails[pl.ds(0, size), :], low[cols, :], over,
                preferred_element_type=jnp.float32,
            )
            partial[pl.ds(starts[c], size), cols] = both[:size] + (both[size:] + rest)
            return carry

        lax.fori_loop(0, instruments // width, column, 0)

    def pair_copy(c, slot, p):
        _, _, _, take = plan[c]
        cols = pl.ds(pl.multiple_of(p * piece, piece), piece)
        away = starts[c] + (slot * CORES + (1 - core)) * take
        return pltpu.make_async_remote_copy(
            partial.at[pl.ds(pl.multiple_of(away, 8), take), cols],
            pair_buf.at[pl.ds(pl.multiple_of(starts[c] // 2 + slot * take, 8), take), cols],
            pair_send.at[c, slot, p],
            pair_recv.at[c, slot, p],
            device_id={"scen": z * CORES + (1 - core)},
        )

    def scale_and_pair(c):
        _, _, _, take = plan[c]
        for i in range(1, scens):
            stats_copy(c, i).wait_recv()
        peak = stats[c, 0, 0:1, :]
        for i in range(1, scens):
            peak = jnp.maximum(peak, stats[c, i, 0:1, :])
        total = stats[c, 0, 1:2, :] * jnp.exp(stats[c, 0, 0:1, :] - peak)
        for i in range(1, scens):
            total = total + stats[c, i, 1:2, :] * jnp.exp(stats[c, i, 0:1, :] - peak)
        scale = -jnp.exp(stats[c, 0, 0:1, :] - peak) / total
        factor[...] = jnp.transpose(jnp.broadcast_to(scale, (LANES, LANES)))
        value = jnp.broadcast_to(peak + jnp.log(total) - math.log(total_scen), (8, LANES))
        lane = lax.broadcasted_iota(jnp.int32, (8, LANES), 1)
        for slot in range(2):
            for k in range(CORES):
                account = (owner_of(c, slot) * CORES + k) * rows + plan[c][2]
                line, at = account // LANES, account % LANES
                src = (slot * CORES + k) * take
                moved = pltpu.roll(value, (at - src) % LANES, 1)
                keep = jnp.logical_and(lane >= at, lane < at + take)
                marg[line : line + 1, :] = jnp.where(keep, moved, marg[line : line + 1, :])[0:1, :]

        def column(p, carry):
            cols = pl.ds(pl.multiple_of(p * piece, piece), piece)
            for g in range(4 * take // 8):
                lines = pl.ds(starts[c] + g * 8, 8)
                partial[lines, cols] = partial[lines, cols] * factor[pl.ds(g * 8, 8), 0:1]
            pair_copy(c, far, p).start()
            pair_copy(c, 1 - far, p).start()
            return carry

        lax.fori_loop(0, pieces, column, 0)

    def mine_at(c, slot, p):
        _, _, _, take = plan[c]
        cols = pl.ds(pl.multiple_of(p * piece, piece), piece)
        return pl.ds(pl.multiple_of(starts[c] + (slot * CORES + core) * take, 8), take), cols

    def there_at(c, slot, p):
        _, _, _, take = plan[c]
        cols = pl.ds(pl.multiple_of(p * piece, piece), piece)
        return pl.ds(pl.multiple_of(starts[c] // 2 + slot * take, 8), take), cols

    def line_copy(c, slot, p, way):
        lines, cols = mine_at(c, slot, p)
        there, _ = there_at(c, slot, p)
        return pltpu.make_async_remote_copy(
            partial.at[lines, cols],
            line_buf.at[way, there, cols],
            line_send.at[c, slot, p],
            line_recv.at[way, c, slot, p],
            device_id={"scen": me + CORES if way == 0 else me - CORES},
        )

    def join_pair(c):
        for slot in (far, 1 - far):
            owner = owner_of(c, slot)

            def step(p, carry):
                lines, cols = mine_at(c, slot, p)
                there, _ = there_at(c, slot, p)
                pair_copy(c, slot, p).wait_recv()
                partial[lines, cols] += pair_buf[there, cols]

                @pl.when(jnp.logical_and(z == 0, owner > 0))
                def _():
                    line_copy(c, slot, p, 0).start()

                @pl.when(jnp.logical_and(z == chips - 1, owner < chips - 1))
                def _():
                    line_copy(c, slot, p, 1).start()

                return carry

            lax.fori_loop(0, pieces, step, 0)

    def forward(c):
        for slot in (far, 1 - far):
            owner = owner_of(c, slot)
            up = jnp.logical_and(z > 0, owner > z)
            down = jnp.logical_and(z < chips - 1, owner < z)
            for way, here in ((0, up), (1, down)):

                @pl.when(here)
                def _():
                    def step(p, carry):
                        lines, cols = mine_at(c, slot, p)
                        there, _ = there_at(c, slot, p)
                        copy = line_copy(c, slot, p, way)
                        copy.wait_recv()
                        partial[lines, cols] += line_buf[way, there, cols]
                        copy.start()
                        return carry

                    lax.fori_loop(0, pieces, step, 0)

    def finish(c):
        _, _, first, take = plan[c]
        for slot in range(2):
            owner = owner_of(c, slot)

            @pl.when(z == owner)
            def _():
                def step(p, carry):
                    lines, cols = mine_at(c, slot, p)
                    there, _ = there_at(c, slot, p)
                    if owner == 0:
                        line_copy(c, slot, p, 1).wait_recv()
                        value = partial[lines, cols] + line_buf[1, there, cols]
                    elif owner == chips - 1:
                        line_copy(c, slot, p, 0).wait_recv()
                        value = partial[lines, cols] + line_buf[0, there, cols]
                    else:
                        line_copy(c, slot, p, 0).wait_recv()
                        value = partial[lines, cols] + line_buf[0, there, cols]
                        line_copy(c, slot, p, 1).wait_recv()
                        value = value + line_buf[1, there, cols]
                    gradient_out[pl.ds(first, take), cols] = value
                    return carry

                lax.fori_loop(0, pieces, step, 0)

    pl.semaphore_wait(barrier, insts - 1 + scens - 1)
    send_parts(0)
    sum_and_gather(0)
    send_parts(1)
    if number > 2:
        profit(2)
    for c in range(number):
        weigh(c)
        multiply(c)
        if c + 1 < number:
            sum_and_gather(c + 1)
        scale_and_pair(c)
        if c == 0 and number > 2:
            send_parts(2)
        join_pair(c)
        if c > 0:
            forward(c - 1)
            if c + 2 < number:
                profit(c + 2)
                send_parts(c + 2)
    for c in range(number - 1):
        finish(c)
    forward(number - 1)
    finish(number - 1)

    share = accounts // insts
    if share % LANES == 0:
        margin_out[...] = marg[pl.ds(inst * (share // LANES), share // LANES), :]
    else:
        margin_out[...] = marg[pl.ds(inst * share // LANES, 1), :]

    for c in range(number):
        for i in range(1, insts):
            rs_copy(c, i).wait_send()
            ag_copy(c, i, inst).wait_send()
        for i in range(1, scens):
            stats_copy(c, i).wait_send()
        for slot in range(2):
            owner = owner_of(c, slot)

            def drain(p, carry):
                pair_copy(c, slot, p).wait_send()

                @pl.when(owner > z)
                def _():
                    line_copy(c, slot, p, 0).wait_send()

                @pl.when(owner < z)
                def _():
                    line_copy(c, slot, p, 1).wait_send()

                return carry

            lax.fori_loop(0, pieces, drain, 0)


def body(positions, holding_block_grid, risk):
    accounts, instruments = positions.shape
    scen_here = risk.shape[1]
    insts = lax.axis_size("inst")
    scens = lax.axis_size("scen")
    chips = scens // CORES
    rows = accounts // scens
    softness = 8.0 * math.sqrt(instruments * insts)
    plan = chunk_plan(rows, chips, insts)
    number = len(plan)
    share = accounts // insts
    most = max(4 * take for _, _, _, take in plan)
    head = 4 * (plan[0][3] + plan[1][3])
    pieces = instruments // min(PIECE, instruments)
    kblock = min(512, instruments)
    cfg = (plan, accounts, insts, scens, softness, scen_here * scens)
    dma = pltpu.SemaphoreType.DMA
    margin, gradient = pl.pallas_call(
        functools.partial(kernel, cfg),
        out_shape=(
            jax.ShapeDtypeStruct((max(1, share // LANES), LANES), jnp.float32),
            jax.ShapeDtypeStruct((rows, instruments), jnp.float32),
        ),
        in_specs=[
            pl.BlockSpec(memory_space=pl.ANY),
            pl.BlockSpec(memory_space=pltpu.SMEM),
            pl.BlockSpec(memory_space=pl.ANY),
        ],
        out_specs=(
            pl.BlockSpec(memory_space=pltpu.VMEM),
            pl.BlockSpec(memory_space=pltpu.VMEM),
        ),
        scratch_shapes=[
            pltpu.VMEM((STAGES, kblock, scen_here), jnp.float32),
            pltpu.VMEM((2, max(most, head), instruments), jnp.int32),
            pltpu.VMEM((max(most, head), instruments), jnp.bfloat16),
            pltpu.VMEM((instruments, scen_here), jnp.bfloat16),
            pltpu.VMEM((instruments, scen_here), jnp.bfloat16),
            pltpu.VMEM((accounts, scen_here), jnp.float32),
            pltpu.VMEM((insts - 1, accounts // insts, scen_here), jnp.float32),
            pltpu.VMEM((accounts, scen_here), jnp.float32),
            pltpu.VMEM((2 * most, scen_here), jnp.bfloat16),
            pltpu.VMEM((LANES, LANES), jnp.float32),
            pltpu.VMEM((LANES, LANES), jnp.float32),
            pltpu.VMEM((number, scens, 2, LANES), jnp.float32),
            pltpu.VMEM((LANES, LANES), jnp.float32),
            pltpu.VMEM((accounts, instruments), jnp.float32),
            pltpu.VMEM((accounts // 2, instruments), jnp.float32),
            pltpu.VMEM((2, accounts // 2, instruments), jnp.float32),
            pltpu.VMEM((max(8, accounts // LANES), LANES), jnp.float32),
            dma((STAGES,)),
            dma((2, 2, 4)),
            dma((number, insts - 1)),
            dma((number, insts - 1)),
            dma((number, insts - 1)),
            dma((number, insts - 1)),
            dma((number, scens - 1)),
            dma((number, scens - 1)),
            dma((number, 2, pieces)),
            dma((number, 2, pieces)),
            dma((number, 2, pieces)),
            dma((2, number, 2, pieces)),
        ],
        compiler_params=pltpu.CompilerParams(
            collective_id=0, has_side_effects=True, vmem_limit_bytes=67043328
        ),
    )(positions, holding_block_grid, risk)
    if share % LANES == 0:
        margin = margin.reshape(share)
    else:
        start = (lax.axis_index("inst") * share) % LANES
        margin = lax.dynamic_slice_in_dim(margin.reshape(LANES), start, share)
    return (margin, gradient)


def solution(mesh):
    placed = (P(None, "inst"), P(None, "inst"), P("inst", "scen"))
    return jax.shard_map(
        body, mesh=mesh, in_specs=placed, out_specs=(P("inst"), P("scen", "inst")), check_vma=False
    )
```

```python
import functools
import math

import jax
import jax.numpy as jnp
from jax import lax
from jax.experimental import pallas as pl
from jax.experimental.pallas import tpu as pltpu
from jax.sharding import PartitionSpec as P

ABLK = 64
IBLK = 128
CORES = 2
LANES = 128
STAGES = 3
PIECE = 1024
STRIP = 16


def chunk_plan(rows, chips, inst_number):
    unit = max(16, 2 * inst_number)
    inner, outer = [], []
    for phase in range(chips // 2):
        done = 0
        last = phase == chips // 2 - 1
        while done < rows:
            take = min(unit if last and done < 2 * unit else 2 * unit, rows - done)
            (inner if last else outer).append((chips - 1 - phase, phase, done, take))
            done += take
    return inner[:2] + outer + inner[2:]


def kernel(
    cfg,
    positions,
    grid,
    risk,
    margin_out,
    gradient_out,
    stage,
    pos_buf,
    held,
    high,
    low,
    part,
    rs_buf,
    full,
    tails,
    peaks,
    totals,
    stats,
    factor,
    line_factor,
    partial,
    pair_buf,
    line_buf,
    marg,
    stage_sem,
    pos_sem,
    rs_send,
    rs_recv,
    ag_send,
    ag_recv,
    stats_send,
    stats_recv,
    pair_send,
    pair_recv,
    line_send,
    line_recv,
):
    plan, accounts, insts, scens, softness, total_scen = cfg
    instruments, scen_here = risk.shape
    rows = accounts // scens
    chips = scens // CORES
    piece = min(PIECE, instruments)
    pieces = instruments // piece
    kblock = stage.shape[1]
    kblocks = instruments // kblock
    number = len(plan)
    inst = lax.axis_index("inst")
    me = lax.axis_index("scen")
    z = me // CORES
    core = me % CORES
    far = z // (chips // 2)

    sizes = [4 * take for _, _, _, take in plan]
    starts = [sum(sizes[:c]) for c in range(number)]
    head = sizes[0] + sizes[1]

    def owner_of(c, slot):
        above, below, _, _ = plan[c]
        return above - slot * (above - below)

    def load_risk(b):
        slot = b % STAGES
        return pltpu.make_async_copy(
            risk.at[pl.ds(b * kblock, kblock), :], stage.at[slot], stage_sem.at[slot]
        )

    def pos_copies(c, slot, base):
        _, _, first, take = plan[c]
        copies = []
        for s in range(2):
            for k in range(CORES):
                account = (owner_of(c, s) * CORES + k) * rows + first
                group = s * CORES + k
                copies.append(
                    pltpu.make_async_copy(
                        positions.at[pl.ds(account, take), :],
                        pos_buf.at[slot, pl.ds(base + group * take, take), :],
                        pos_sem.at[slot, base // sizes[0] if base else 0, group],
                    )
                )
        return copies

    def make_held(c, slot, base, shift=0):
        _, _, first, take = plan[c]

        def column(j, carry):
            cols = pl.ds(pl.multiple_of(j * IBLK, IBLK), IBLK)
            for s in range(2):
                for k in range(CORES):
                    account = (owner_of(c, s) * CORES + k) * rows + first
                    live = grid[account // ABLK, j].astype(jnp.float32)
                    lines = pl.ds(base + (s * CORES + k) * take, take)
                    held[pl.ds(shift + base + (s * CORES + k) * take, take), cols] = (
                        pos_buf[slot, lines, cols].astype(jnp.float32) * live
                    ).astype(jnp.bfloat16)
            return carry

        lax.fori_loop(0, instruments // IBLK, column, 0)

    for copy in pos_copies(0, 0, 0) + pos_copies(1, 0, sizes[0]):
        copy.start()
    for b in range(min(STAGES, kblocks)):
        load_risk(b).start()
    if number > 2:
        for copy in pos_copies(2, 1, 0):
            copy.start()

    barrier = pltpu.get_barrier_semaphore()
    for i in range(1, insts):
        pl.semaphore_signal(barrier, inc=1, device_id={"inst": (inst + i) % insts})
    for i in range(1, scens):
        pl.semaphore_signal(barrier, inc=1, device_id={"scen": (me + i) % scens})

    peaks[...] = jnp.zeros_like(peaks)
    totals[...] = jnp.ones_like(totals)
    marg[...] = jnp.zeros_like(marg)
    part[pl.ds(0, head), :] = jnp.zeros((head, scen_here), jnp.float32)

    for copy in pos_copies(0, 0, 0) + pos_copies(1, 0, sizes[0]):
        copy.wait()
    make_held(0, 0, 0)
    make_held(1, 0, sizes[0])
    if number > 3:
        for copy in pos_copies(3, 0, 0):
            copy.start()

    def arrive(b, carry):
        slot = b % STAGES
        load_risk(b).wait()

        def split(r, inner):
            lines = pl.ds(pl.multiple_of(r * STRIP, STRIP), STRIP)
            value = stage[slot, lines, :]
            top = value.astype(jnp.bfloat16)
            there = pl.ds(pl.multiple_of(b * kblock + r * STRIP, STRIP), STRIP)
            high[there, :] = top
            low[there, :] = (value - top.astype(jnp.float32)).astype(jnp.bfloat16)
            return inner

        lax.fori_loop(0, kblock // STRIP, split, 0, unroll=2)

        @pl.when(b + STAGES < kblocks)
        def _():
            load_risk(b + STAGES).start()

        deep = pl.ds(pl.multiple_of(b * kblock, kblock), kblock)
        mine = held[pl.ds(0, head), deep]
        part[pl.ds(0, head), :] += jnp.dot(
            mine, high[deep, :], preferred_element_type=jnp.float32
        ) + jnp.dot(mine, low[deep, :], preferred_element_type=jnp.float32)
        return carry

    lax.fori_loop(0, kblocks, arrive, 0)

    width = min(256, scen_here)
    blocks = scen_here // width
    shifted = pos_buf.shape[1]

    def profit_load(c):
        slot = (c - 1) % 2
        for copy in pos_copies(c, slot, 0):
            copy.wait()
        make_held(c, slot, 0, c % 2 * shifted)
        if c + 2 < number:
            for copy in pos_copies(c + 2, slot, 0):
                copy.start()

    def profit(c, begin, end):
        def column(n, carry):
            cols = pl.ds(pl.multiple_of(n * width, width), width)
            mine = held[pl.ds(c % 2 * shifted, sizes[c]), :]
            part[pl.ds(starts[c], sizes[c]), cols] = jnp.dot(
                mine, high[:, cols], preferred_element_type=jnp.float32
            ) + jnp.dot(mine, low[:, cols], preferred_element_type=jnp.float32)
            return carry

        lax.fori_loop(begin, end, column, 0)

    def rs_copy(c, i):
        group = sizes[c] // insts
        to = (inst + i) % insts
        return pltpu.make_async_remote_copy(
            part.at[pl.ds(pl.multiple_of(starts[c] + to * group, 8), group), :],
            rs_buf.at[i - 1, pl.ds(starts[c] // insts, group), :],
            rs_send.at[c, i - 1],
            rs_recv.at[c, i - 1],
            device_id={"inst": to},
        )

    def ag_copy(c, i, source):
        group = sizes[c] // insts
        lines = pl.ds(pl.multiple_of(starts[c] + source * group, 8), group)
        return pltpu.make_async_remote_copy(
            full.at[lines, :],
            full.at[lines, :],
            ag_send.at[c, i - 1],
            ag_recv.at[c, i - 1],
            device_id={"inst": (inst + i) % insts},
        )

    def send_parts(c):
        for i in range(1, insts):
            rs_copy(c, i).start()

    def sum_and_gather(c):
        group = sizes[c] // insts
        lines = pl.ds(pl.multiple_of(starts[c] + inst * group, 8), group)
        value = part[lines, :]
        for i in range(1, insts):
            rs_copy(c, i).wait_recv()
            value = value + rs_buf[i - 1, pl.ds(starts[c] // insts, group), :]
        full[lines, :] = value
        for i in range(1, insts):
            ag_copy(c, i, inst).start()

    def stats_copy(c, i):
        return pltpu.make_async_remote_copy(
            stats.at[c, 0],
            stats.at[c, i],
            stats_send.at[c, i - 1],
            stats_recv.at[c, i - 1],
            device_id={"scen": (me + i) % scens},
        )

    def weigh(c):
        size = sizes[c]
        for i in range(1, insts):
            ag_copy(c, i, (inst + insts - i) % insts).wait_recv()

        def strip(r, carry):
            lines = pl.ds(pl.multiple_of(r * STRIP, STRIP), STRIP)
            score = full[pl.ds(pl.multiple_of(starts[c] + r * STRIP, STRIP), STRIP), :] * (
                -1.0 / softness
            )
            peak = jnp.max(score, axis=1, keepdims=True)
            tail = jnp.exp(score - peak)
            total = jnp.sum(tail, axis=1, keepdims=True)
            top = tail.astype(jnp.bfloat16)
            tails[lines, :] = top
            tails[pl.ds(pl.multiple_of(size + r * STRIP, STRIP), STRIP), :] = (
                tail - top.astype(jnp.float32)
            ).astype(jnp.bfloat16)
            peaks[lines, :] = jnp.broadcast_to(peak, (STRIP, LANES))
            totals[lines, :] = jnp.broadcast_to(total, (STRIP, LANES))
            return carry

        lax.fori_loop(0, size // STRIP, strip, 0)
        stats[c, 0, 0:1, :] = jnp.transpose(peaks[...])[0:1, :]
        stats[c, 0, 1:2, :] = jnp.transpose(totals[...])[0:1, :]
        for i in range(1, scens):
            stats_copy(c, i).start()

    def pair_copy(c, slot, p):
        _, _, _, take = plan[c]
        cols = pl.ds(pl.multiple_of(p * piece, piece), piece)
        away = starts[c] + (slot * CORES + (1 - core)) * take
        return pltpu.make_async_remote_copy(
            partial.at[pl.ds(pl.multiple_of(away, 8), take), cols],
            pair_buf.at[pl.ds(pl.multiple_of(starts[c] // 2 + slot * take, 8), take), cols],
            pair_send.at[c, slot, p],
            pair_recv.at[c, slot, p],
            device_id={"scen": z * CORES + (1 - core)},
        )

    peer = 1 + (1 - core) * (scens - 2)

    def columns_of(values):
        line = lax.broadcasted_iota(jnp.int32, (LANES, LANES), 0)
        table = jnp.zeros((LANES, LANES), jnp.float32)
        for n, value in enumerate(values):
            table = jnp.where(line == n, jnp.broadcast_to(value, (LANES, LANES)), table)
        return jnp.transpose(table)

    def pair_factors(c):
        stats_copy(c, peer).wait_recv()
        mine = stats[c, 0, 0:1, :]
        other = stats[c, peer, 0:1, :]
        both = jnp.maximum(mine, other)
        factor[...] = columns_of([-jnp.exp(mine - both), -jnp.exp(other - both)])

    def multiply(c, begin, end):
        size = sizes[c]
        over = (((1,), (1,)), ((), ()))

        def column(p, carry):
            @pl.when(p < pieces)
            def _():
                cols = pl.ds(pl.multiple_of(p * piece, piece), piece)
                both = lax.dot_general(
                    tails[pl.ds(0, 2 * size), :], high[cols, :], over,
                    preferred_element_type=jnp.float32,
                )
                rest = lax.dot_general(
                    tails[pl.ds(0, size), :], low[cols, :], over,
                    preferred_element_type=jnp.float32,
                )
                partial[pl.ds(starts[c], size), cols] = both[:size] + (both[size:] + rest)
                pair_copy(c, far, p).start()
                pair_copy(c, 1 - far, p).start()

            @pl.when(p == 1)
            def _():
                pair_factors(c)

            @pl.when(p > 0)
            def _():
                join_pair(c, p - 1)

            return carry

        lax.fori_loop(begin, end, column, 0)

    def settle(c):
        _, _, first, take = plan[c]
        for i in range(1, scens):

            @pl.when(peer != i)
            def _():
                stats_copy(c, i).wait_recv()

        lowest = jnp.full((1, LANES), -3e38, jnp.float32)
        below, here, above = lowest, lowest, lowest
        for i in range(scens):
            chip = ((me + scens - i) % scens) // CORES
            value = stats[c, i, 0:1, :]
            below = jnp.maximum(below, jnp.where(chip < z, value, lowest))
            here = jnp.maximum(here, jnp.where(chip == z, value, lowest))
            above = jnp.maximum(above, jnp.where(chip > z, value, lowest))
        peak = jnp.maximum(jnp.maximum(below, above), here)
        total = jnp.zeros((1, LANES), jnp.float32)
        for i in range(scens):
            total = total + stats[c, i, 1:2, :] * jnp.exp(stats[c, i, 0:1, :] - peak)
        up, down = jnp.maximum(below, here), jnp.maximum(above, here)
        line_factor[c] = columns_of(
            [
                jnp.exp(here - up),
                jnp.exp(below - up),
                jnp.exp(here - down),
                jnp.exp(above - down),
                jnp.exp(here - peak) / total,
                jnp.exp(below - peak) / total,
                jnp.exp(above - peak) / total,
            ]
        )
        value = jnp.broadcast_to(peak + jnp.log(total) - math.log(total_scen), (8, LANES))
        lane = lax.broadcasted_iota(jnp.int32, (8, LANES), 1)
        for slot in range(2):
            for k in range(CORES):
                account = (owner_of(c, slot) * CORES + k) * rows + first
                line, at = account // LANES, account % LANES
                src = (slot * CORES + k) * take
                moved = pltpu.roll(value, (at - src) % LANES, 1)
                keep = jnp.logical_and(lane >= at, lane < at + take)
                marg[line : line + 1, :] = jnp.where(keep, moved, marg[line : line + 1, :])[0:1, :]

    def mine_at(c, slot, p):
        _, _, _, take = plan[c]
        cols = pl.ds(pl.multiple_of(p * piece, piece), piece)
        return pl.ds(pl.multiple_of(starts[c] + (slot * CORES + core) * take, 8), take), cols

    def there_at(c, slot, p):
        _, _, _, take = plan[c]
        cols = pl.ds(pl.multiple_of(p * piece, piece), piece)
        return pl.ds(pl.multiple_of(starts[c] // 2 + slot * take, 8), take), cols

    def line_copy(c, slot, p, way):
        lines, cols = mine_at(c, slot, p)
        there, _ = there_at(c, slot, p)
        return pltpu.make_async_remote_copy(
            partial.at[lines, cols],
            line_buf.at[way, there, cols],
            line_send.at[c, slot, p],
            line_recv.at[way, c, slot, p],
            device_id={"scen": me + CORES if way == 0 else me - CORES},
        )

    def own_factor(c, slot, n):
        _, _, _, take = plan[c]
        lines = pl.ds(pl.multiple_of((slot * CORES + core) * take, 8), take)
        return line_factor[c, lines, n : n + 1]

    def join_pair(c, p):
        _, _, _, take = plan[c]
        for slot in (far, 1 - far):
            owner = owner_of(c, slot)
            lines, cols = mine_at(c, slot, p)
            there, _ = there_at(c, slot, p)
            these = pl.ds(pl.multiple_of((slot * CORES + core) * take, 8), take)
            pair_copy(c, slot, p).wait_recv()
            partial[lines, cols] = (
                partial[lines, cols] * factor[these, 0:1] + pair_buf[there, cols] * factor[these, 1:2]
            )

            @pl.when(jnp.logical_and(z == 0, owner > 0))
            def _():
                line_copy(c, slot, p, 0).start()

            @pl.when(jnp.logical_and(z == chips - 1, owner < chips - 1))
            def _():
                line_copy(c, slot, p, 1).start()

    def forward(c, order):
        slot = far if order == 0 else 1 - far
        if order == 0:
            settle(c)
        owner = owner_of(c, slot)
        up = jnp.logical_and(z > 0, owner > z)
        down = jnp.logical_and(z < chips - 1, owner < z)
        for way, here in ((0, up), (1, down)):

            @pl.when(here)
            def _():
                def step(p, carry):
                    lines, cols = mine_at(c, slot, p)
                    there, _ = there_at(c, slot, p)
                    copy = line_copy(c, slot, p, way)
                    copy.wait_recv()
                    partial[lines, cols] = partial[lines, cols] * own_factor(
                        c, slot, 2 * way
                    ) + line_buf[way, there, cols] * own_factor(c, slot, 2 * way + 1)
                    copy.start()
                    return carry

                lax.fori_loop(0, pieces, step, 0)

    def finish(c):
        _, _, first, take = plan[c]
        for slot in range(2):
            owner = owner_of(c, slot)

            @pl.when(z == owner)
            def _():
                def step(p, carry):
                    lines, cols = mine_at(c, slot, p)
                    there, _ = there_at(c, slot, p)
                    value = partial[lines, cols] * own_factor(c, slot, 4)
                    for way in range(2):
                        if (way == 0 and owner > 0) or (way == 1 and owner < chips - 1):
                            line_copy(c, slot, p, way).wait_recv()
                            value = value + line_buf[way, there, cols] * own_factor(c, slot, 5 + way)
                    gradient_out[pl.ds(first, take), cols] = value
                    return carry

                lax.fori_loop(0, pieces, step, 0)

    pl.semaphore_wait(barrier, insts - 1 + scens - 1)
    send_parts(0)
    send_parts(1)
    if number > 2:
        profit_load(2)
        profit(2, 0, blocks)
    if number > 4:
        profit_load(4)
        profit(4, 0, blocks // 2)
    sum_and_gather(0)
    if number > 2:
        send_parts(2)
    if number > 3:
        profit_load(3)
        profit(3, 0, blocks)
    if number > 4:
        profit(4, blocks // 2, blocks)
    sum_and_gather(1)
    if number > 3:
        send_parts(3)
    half = (pieces + 1) // 2
    for c in range(number):
        weigh(c)
        multiply(c, 0, half)
        if c + 2 < number:
            sum_and_gather(c + 2)
        if c + 4 < number:
            send_parts(c + 4)
        if c >= 4:
            forward(c - 2, 1)
        multiply(c, half, pieces + 1)
        if c + 5 < number:
            profit_load(c + 5)
            profit(c + 5, 0, blocks)
        if c == 2:
            for n in (0, 1):
                forward(n, 0)
                forward(n, 1)
        if c >= 3:
            forward(c - 1, 0)
    if number >= 4:
        forward(number - 2, 1)
    for c in range(number - 2):
        finish(c)
    forward(number - 1, 0)
    forward(number - 1, 1)
    finish(number - 2)
    finish(number - 1)

    share = accounts // insts
    if share % LANES == 0:
        margin_out[...] = marg[pl.ds(inst * (share // LANES), share // LANES), :]
    else:
        margin_out[...] = marg[pl.ds(inst * share // LANES, 1), :]

    for c in range(number):
        for i in range(1, insts):
            rs_copy(c, i).wait_send()
            ag_copy(c, i, inst).wait_send()
        for i in range(1, scens):
            stats_copy(c, i).wait_send()
        for slot in range(2):
            owner = owner_of(c, slot)

            def drain(p, carry):
                pair_copy(c, slot, p).wait_send()

                @pl.when(owner > z)
                def _():
                    line_copy(c, slot, p, 0).wait_send()

                @pl.when(owner < z)
                def _():
                    line_copy(c, slot, p, 1).wait_send()

                return carry

            lax.fori_loop(0, pieces, drain, 0)


def body(positions, holding_block_grid, risk):
    accounts, instruments = positions.shape
    scen_here = risk.shape[1]
    insts = lax.axis_size("inst")
    scens = lax.axis_size("scen")
    chips = scens // CORES
    rows = accounts // scens
    softness = 8.0 * math.sqrt(instruments * insts)
    plan = chunk_plan(rows, chips, insts)
    number = len(plan)
    share = accounts // insts
    most = max(4 * take for _, _, _, take in plan)
    head = 4 * (plan[0][3] + plan[1][3])
    pieces = instruments // min(PIECE, instruments)
    kblock = min(512, instruments)
    cfg = (plan, accounts, insts, scens, softness, scen_here * scens)
    dma = pltpu.SemaphoreType.DMA
    margin, gradient = pl.pallas_call(
        functools.partial(kernel, cfg),
        out_shape=(
            jax.ShapeDtypeStruct((max(1, share // LANES), LANES), jnp.float32),
            jax.ShapeDtypeStruct((rows, instruments), jnp.float32),
        ),
        in_specs=[
            pl.BlockSpec(memory_space=pl.ANY),
            pl.BlockSpec(memory_space=pltpu.SMEM),
            pl.BlockSpec(memory_space=pl.ANY),
        ],
        out_specs=(
            pl.BlockSpec(memory_space=pltpu.VMEM),
            pl.BlockSpec(memory_space=pltpu.VMEM),
        ),
        scratch_shapes=[
            pltpu.VMEM((STAGES, kblock, scen_here), jnp.float32),
            pltpu.VMEM((2, max(most, head), instruments), jnp.int32),
            pltpu.VMEM((2 * max(most, head), instruments), jnp.bfloat16),
            pltpu.VMEM((instruments, scen_here), jnp.bfloat16),
            pltpu.VMEM((instruments, scen_here), jnp.bfloat16),
            pltpu.VMEM((accounts, scen_here), jnp.float32),
            pltpu.VMEM((insts - 1, accounts // insts, scen_here), jnp.float32),
            pltpu.VMEM((accounts, scen_here), jnp.float32),
            pltpu.VMEM((2 * most, scen_here), jnp.bfloat16),
            pltpu.VMEM((LANES, LANES), jnp.float32),
            pltpu.VMEM((LANES, LANES), jnp.float32),
            pltpu.VMEM((number, scens, 2, LANES), jnp.float32),
            pltpu.VMEM((LANES, LANES), jnp.float32),
            pltpu.VMEM((number, LANES, LANES), jnp.float32),
            pltpu.VMEM((accounts, instruments), jnp.float32),
            pltpu.VMEM((accounts // 2, instruments), jnp.float32),
            pltpu.VMEM((2, accounts // 2, instruments), jnp.float32),
            pltpu.VMEM((max(8, accounts // LANES), LANES), jnp.float32),
            dma((STAGES,)),
            dma((2, 2, 4)),
            dma((number, insts - 1)),
            dma((number, insts - 1)),
            dma((number, insts - 1)),
            dma((number, insts - 1)),
            dma((number, scens - 1)),
            dma((number, scens - 1)),
            dma((number, 2, pieces)),
            dma((number, 2, pieces)),
            dma((number, 2, pieces)),
            dma((2, number, 2, pieces)),
        ],
        compiler_params=pltpu.CompilerParams(
            collective_id=0, has_side_effects=True, vmem_limit_bytes=67043328
        ),
    )(positions, holding_block_grid, risk)
    if share % LANES == 0:
        margin = margin.reshape(share)
    else:
        start = (lax.axis_index("inst") * share) % LANES
        margin = lax.dynamic_slice_in_dim(margin.reshape(LANES), start, share)
    return (margin, gradient)


def solution(mesh):
    placed = (P(None, "inst"), P(None, "inst"), P("inst", "scen"))
    return jax.shard_map(
        body, mesh=mesh, in_specs=placed, out_specs=(P("inst"), P("scen", "inst")), check_vma=False
    )
```

```python
import functools
import math

import jax
import jax.numpy as jnp
from jax import lax
from jax.experimental import pallas as pl
from jax.experimental.pallas import tpu as pltpu
from jax.sharding import PartitionSpec as P

ABLK = 64
IBLK = 128
CORES = 2
LANES = 128
STAGES = 3
PIECE = 1024
STRIP = 16
SPLIT = 64


def chunk_plan(rows, chips, inst_number):
    unit = max(16, 2 * inst_number)
    inner, outer = [], []
    for phase in range(chips // 2):
        done = 0
        last = phase == chips // 2 - 1
        while done < rows:
            take = min(unit if last and done < 2 * unit else 2 * unit, rows - done)
            (inner if last else outer).append((chips - 1 - phase, phase, done, take))
            done += take
    return inner[:2] + outer + inner[2:]


def kernel(
    cfg,
    positions,
    grid,
    risk,
    margin_out,
    gradient_out,
    stage,
    pos_buf,
    held,
    high,
    low,
    part,
    rs_buf,
    full,
    tails,
    peaks,
    totals,
    stats,
    factor,
    line_factor,
    partial,
    pair_buf,
    line_buf,
    marg,
    stage_sem,
    pos_sem,
    rs_send,
    rs_recv,
    ag_send,
    ag_recv,
    stats_send,
    stats_recv,
    pair_send,
    pair_recv,
    line_send,
    line_recv,
):
    plan, accounts, insts, scens, softness, total_scen = cfg
    instruments, scen_here = risk.shape
    rows = accounts // scens
    chips = scens // CORES
    piece = min(PIECE, instruments)
    pieces = instruments // piece
    kblock = stage.shape[1]
    kblocks = instruments // kblock
    number = len(plan)
    inst = lax.axis_index("inst")
    me = lax.axis_index("scen")
    z = me // CORES
    core = me % CORES
    far = z // (chips // 2)

    sizes = [4 * take for _, _, _, take in plan]
    starts = [sum(sizes[:c]) for c in range(number)]
    head = sizes[0] + sizes[1]

    def owner_of(c, slot):
        above, below, _, _ = plan[c]
        return above - slot * (above - below)

    def load_risk(b):
        slot = b % STAGES
        return pltpu.make_async_copy(
            risk.at[pl.ds(b * kblock, kblock), :], stage.at[slot], stage_sem.at[slot]
        )

    def pos_copies(c, slot, base):
        _, _, first, take = plan[c]
        copies = []
        for s in range(2):
            for k in range(CORES):
                account = (owner_of(c, s) * CORES + k) * rows + first
                group = s * CORES + k
                copies.append(
                    pltpu.make_async_copy(
                        positions.at[pl.ds(account, take), :],
                        pos_buf.at[slot, pl.ds(base + group * take, take), :],
                        pos_sem.at[slot, base // sizes[0] if base else 0, group],
                    )
                )
        return copies

    def make_held(c, slot, base, shift=0):
        _, _, first, take = plan[c]

        def column(j, carry):
            cols = pl.ds(pl.multiple_of(j * IBLK, IBLK), IBLK)
            for s in range(2):
                for k in range(CORES):
                    account = (owner_of(c, s) * CORES + k) * rows + first
                    live = grid[account // ABLK, j].astype(jnp.float32)
                    lines = pl.ds(base + (s * CORES + k) * take, take)
                    held[pl.ds(shift + base + (s * CORES + k) * take, take), cols] = (
                        pos_buf[slot, lines, cols].astype(jnp.float32) * live
                    ).astype(jnp.bfloat16)
            return carry

        lax.fori_loop(0, instruments // IBLK, column, 0)

    for copy in pos_copies(0, 0, 0) + pos_copies(1, 0, sizes[0]):
        copy.start()
    for b in range(min(STAGES, kblocks)):
        load_risk(b).start()
    if number > 2:
        for copy in pos_copies(2, 1, 0):
            copy.start()

    barrier = pltpu.get_barrier_semaphore()
    for i in range(1, insts):
        pl.semaphore_signal(barrier, inc=1, device_id={"inst": (inst + i) % insts})
    for i in range(1, scens):
        pl.semaphore_signal(barrier, inc=1, device_id={"scen": (me + i) % scens})

    peaks[...] = jnp.zeros_like(peaks)
    totals[...] = jnp.ones_like(totals)
    marg[...] = jnp.zeros_like(marg)
    part[pl.ds(0, head), :] = jnp.zeros((head, scen_here), jnp.float32)

    for copy in pos_copies(0, 0, 0) + pos_copies(1, 0, sizes[0]):
        copy.wait()
    make_held(0, 0, 0)
    make_held(1, 0, sizes[0])
    if number > 3:
        for copy in pos_copies(3, 0, 0):
            copy.start()

    def arrive(b, carry):
        slot = b % STAGES
        load_risk(b).wait()

        def split(r, inner):
            lines = pl.ds(pl.multiple_of(r * SPLIT, SPLIT), SPLIT)
            value = stage[slot, lines, :]
            top = value.astype(jnp.bfloat16)
            there = pl.ds(pl.multiple_of(b * kblock + r * SPLIT, SPLIT), SPLIT)
            high[there, :] = top
            low[there, :] = (value - top.astype(jnp.float32)).astype(jnp.bfloat16)
            return inner

        lax.fori_loop(0, kblock // SPLIT, split, 0, unroll=2)

        @pl.when(b + STAGES < kblocks)
        def _():
            load_risk(b + STAGES).start()

        deep = pl.ds(pl.multiple_of(b * kblock, kblock), kblock)
        mine = held[pl.ds(0, head), deep]
        part[pl.ds(0, head), :] += jnp.dot(
            mine, high[deep, :], preferred_element_type=jnp.float32
        ) + jnp.dot(mine, low[deep, :], preferred_element_type=jnp.float32)
        return carry

    lax.fori_loop(0, kblocks, arrive, 0)

    width = min(256, scen_here)
    blocks = scen_here // width
    shifted = pos_buf.shape[1]

    def profit_load(c):
        slot = (c - 1) % 2
        for copy in pos_copies(c, slot, 0):
            copy.wait()
        make_held(c, slot, 0, c % 2 * shifted)
        if c + 2 < number:
            for copy in pos_copies(c + 2, slot, 0):
                copy.start()

    def profit(c, begin, end):
        def column(n, carry):
            cols = pl.ds(pl.multiple_of(n * width, width), width)
            mine = held[pl.ds(c % 2 * shifted, sizes[c]), :]
            part[pl.ds(starts[c], sizes[c]), cols] = jnp.dot(
                mine, high[:, cols], preferred_element_type=jnp.float32
            ) + jnp.dot(mine, low[:, cols], preferred_element_type=jnp.float32)
            return carry

        lax.fori_loop(begin, end, column, 0)

    def rs_copy(c, i):
        group = sizes[c] // insts
        to = (inst + i) % insts
        return pltpu.make_async_remote_copy(
            part.at[pl.ds(pl.multiple_of(starts[c] + to * group, 8), group), :],
            rs_buf.at[i - 1, pl.ds(starts[c] // insts, group), :],
            rs_send.at[c, i - 1],
            rs_recv.at[c, i - 1],
            device_id={"inst": to},
        )

    def ag_copy(c, i, source):
        group = sizes[c] // insts
        lines = pl.ds(pl.multiple_of(starts[c] + source * group, 8), group)
        return pltpu.make_async_remote_copy(
            full.at[lines, :],
            full.at[lines, :],
            ag_send.at[c, i - 1],
            ag_recv.at[c, i - 1],
            device_id={"inst": (inst + i) % insts},
        )

    def send_parts(c):
        for i in range(1, insts):
            rs_copy(c, i).start()

    def sum_and_gather(c):
        group = sizes[c] // insts
        lines = pl.ds(pl.multiple_of(starts[c] + inst * group, 8), group)
        value = part[lines, :]
        for i in range(1, insts):
            rs_copy(c, i).wait_recv()
            value = value + rs_buf[i - 1, pl.ds(starts[c] // insts, group), :]
        full[lines, :] = value
        for i in range(1, insts):
            ag_copy(c, i, inst).start()

    def stats_copy(c, i):
        return pltpu.make_async_remote_copy(
            stats.at[c, 0],
            stats.at[c, i],
            stats_send.at[c, i - 1],
            stats_recv.at[c, i - 1],
            device_id={"scen": (me + i) % scens},
        )

    def weigh(c):
        size = sizes[c]
        for i in range(1, insts):
            ag_copy(c, i, (inst + insts - i) % insts).wait_recv()

        def strip(r, carry):
            lines = pl.ds(pl.multiple_of(r * STRIP, STRIP), STRIP)
            score = full[pl.ds(pl.multiple_of(starts[c] + r * STRIP, STRIP), STRIP), :] * (
                -1.0 / softness
            )
            peak = jnp.max(score, axis=1, keepdims=True)
            tail = jnp.exp(score - peak)
            total = jnp.sum(tail, axis=1, keepdims=True)
            top = tail.astype(jnp.bfloat16)
            tails[lines, :] = top
            tails[pl.ds(pl.multiple_of(size + r * STRIP, STRIP), STRIP), :] = (
                tail - top.astype(jnp.float32)
            ).astype(jnp.bfloat16)
            peaks[lines, :] = jnp.broadcast_to(peak, (STRIP, LANES))
            totals[lines, :] = jnp.broadcast_to(total, (STRIP, LANES))
            return carry

        lax.fori_loop(0, size // STRIP, strip, 0, unroll=2)
        stats[c, 0, 0:1, :] = jnp.transpose(peaks[...])[0:1, :]
        stats[c, 0, 1:2, :] = jnp.transpose(totals[...])[0:1, :]
        for i in range(1, scens):
            stats_copy(c, i).start()

    def pair_copy(c, slot, p):
        _, _, _, take = plan[c]
        cols = pl.ds(pl.multiple_of(p * piece, piece), piece)
        away = starts[c] + (slot * CORES + (1 - core)) * take
        return pltpu.make_async_remote_copy(
            partial.at[pl.ds(pl.multiple_of(away, 8), take), cols],
            pair_buf.at[pl.ds(pl.multiple_of(starts[c] // 2 + slot * take, 8), take), cols],
            pair_send.at[c, slot, p],
            pair_recv.at[c, slot, p],
            device_id={"scen": z * CORES + (1 - core)},
        )

    peer = 1 + (1 - core) * (scens - 2)

    def columns_of(values):
        line = lax.broadcasted_iota(jnp.int32, (LANES, LANES), 0)
        table = jnp.zeros((LANES, LANES), jnp.float32)
        for n, value in enumerate(values):
            table = jnp.where(line == n, jnp.broadcast_to(value, (LANES, LANES)), table)
        return jnp.transpose(table)

    def pair_factors(c):
        stats_copy(c, peer).wait_recv()
        mine = stats[c, 0, 0:1, :]
        other = stats[c, peer, 0:1, :]
        both = jnp.maximum(mine, other)
        factor[...] = columns_of([-jnp.exp(mine - both), -jnp.exp(other - both)])

    def multiply(c, begin, end):
        size = sizes[c]
        over = (((1,), (1,)), ((), ()))

        def column(p, carry):
            @pl.when(p < pieces)
            def _():
                cols = pl.ds(pl.multiple_of(p * piece, piece), piece)
                both = lax.dot_general(
                    tails[pl.ds(0, 2 * size), :], high[cols, :], over,
                    preferred_element_type=jnp.float32,
                )
                rest = lax.dot_general(
                    tails[pl.ds(0, size), :], low[cols, :], over,
                    preferred_element_type=jnp.float32,
                )
                partial[pl.ds(starts[c], size), cols] = both[:size] + (both[size:] + rest)
                pair_copy(c, far, p).start()
                pair_copy(c, 1 - far, p).start()

            @pl.when(p == 1)
            def _():
                pair_factors(c)

            @pl.when(p > 0)
            def _():
                join_pair(c, p - 1)

            return carry

        lax.fori_loop(begin, end, column, 0)

    def settle(c):
        _, _, first, take = plan[c]
        for i in range(1, scens):

            @pl.when(peer != i)
            def _():
                stats_copy(c, i).wait_recv()

        lowest = jnp.full((1, LANES), -3e38, jnp.float32)
        below, here, above = lowest, lowest, lowest
        for i in range(scens):
            chip = ((me + scens - i) % scens) // CORES
            value = stats[c, i, 0:1, :]
            below = jnp.maximum(below, jnp.where(chip < z, value, lowest))
            here = jnp.maximum(here, jnp.where(chip == z, value, lowest))
            above = jnp.maximum(above, jnp.where(chip > z, value, lowest))
        peak = jnp.maximum(jnp.maximum(below, above), here)
        total = jnp.zeros((1, LANES), jnp.float32)
        for i in range(scens):
            total = total + stats[c, i, 1:2, :] * jnp.exp(stats[c, i, 0:1, :] - peak)
        up, down = jnp.maximum(below, here), jnp.maximum(above, here)
        line_factor[c] = columns_of(
            [
                jnp.exp(here - up),
                jnp.exp(below - up),
                jnp.exp(here - down),
                jnp.exp(above - down),
                jnp.exp(here - peak) / total,
                jnp.exp(below - peak) / total,
                jnp.exp(above - peak) / total,
            ]
        )
        value = jnp.broadcast_to(peak + jnp.log(total) - math.log(total_scen), (8, LANES))
        lane = lax.broadcasted_iota(jnp.int32, (8, LANES), 1)
        for slot in range(2):
            for k in range(CORES):
                account = (owner_of(c, slot) * CORES + k) * rows + first
                line, at = account // LANES, account % LANES
                src = (slot * CORES + k) * take
                moved = pltpu.roll(value, (at - src) % LANES, 1)
                keep = jnp.logical_and(lane >= at, lane < at + take)
                marg[line : line + 1, :] = jnp.where(keep, moved, marg[line : line + 1, :])[0:1, :]

    def mine_at(c, slot, p):
        _, _, _, take = plan[c]
        cols = pl.ds(pl.multiple_of(p * piece, piece), piece)
        return pl.ds(pl.multiple_of(starts[c] + (slot * CORES + core) * take, 8), take), cols

    def there_at(c, slot, p):
        _, _, _, take = plan[c]
        cols = pl.ds(pl.multiple_of(p * piece, piece), piece)
        return pl.ds(pl.multiple_of(starts[c] // 2 + slot * take, 8), take), cols

    def line_copy(c, slot, p, way):
        lines, cols = mine_at(c, slot, p)
        there, _ = there_at(c, slot, p)
        return pltpu.make_async_remote_copy(
            partial.at[lines, cols],
            line_buf.at[way, there, cols],
            line_send.at[c, slot, p],
            line_recv.at[way, c, slot, p],
            device_id={"scen": me + CORES if way == 0 else me - CORES},
        )

    def own_factor(c, slot, n):
        _, _, _, take = plan[c]
        lines = pl.ds(pl.multiple_of((slot * CORES + core) * take, 8), take)
        return line_factor[c, lines, n : n + 1]

    def join_pair(c, p):
        _, _, _, take = plan[c]
        for slot in (far, 1 - far):
            owner = owner_of(c, slot)
            lines, cols = mine_at(c, slot, p)
            there, _ = there_at(c, slot, p)
            these = pl.ds(pl.multiple_of((slot * CORES + core) * take, 8), take)
            pair_copy(c, slot, p).wait_recv()
            partial[lines, cols] = (
                partial[lines, cols] * factor[these, 0:1] + pair_buf[there, cols] * factor[these, 1:2]
            )

            @pl.when(jnp.logical_and(z == 0, owner > 0))
            def _():
                line_copy(c, slot, p, 0).start()

            @pl.when(jnp.logical_and(z == chips - 1, owner < chips - 1))
            def _():
                line_copy(c, slot, p, 1).start()

    def forward(c, order, begin, end):
        slot = far if order == 0 else 1 - far
        owner = owner_of(c, slot)
        up = jnp.logical_and(z > 0, owner > z)
        down = jnp.logical_and(z < chips - 1, owner < z)
        for way, here in ((0, up), (1, down)):

            @pl.when(here)
            def _():
                def step(p, carry):
                    lines, cols = mine_at(c, slot, p)
                    there, _ = there_at(c, slot, p)
                    copy = line_copy(c, slot, p, way)
                    copy.wait_recv()
                    partial[lines, cols] = partial[lines, cols] * own_factor(
                        c, slot, 2 * way
                    ) + line_buf[way, there, cols] * own_factor(c, slot, 2 * way + 1)
                    copy.start()
                    return carry

                lax.fori_loop(begin, end, step, 0)

    def finish(c):
        _, _, first, take = plan[c]
        for slot in range(2):
            owner = owner_of(c, slot)

            @pl.when(z == owner)
            def _():
                def step(p, carry):
                    lines, cols = mine_at(c, slot, p)
                    there, _ = there_at(c, slot, p)
                    value = partial[lines, cols] * own_factor(c, slot, 4)
                    for way in range(2):
                        if (way == 0 and owner > 0) or (way == 1 and owner < chips - 1):
                            line_copy(c, slot, p, way).wait_recv()
                            value = value + line_buf[way, there, cols] * own_factor(c, slot, 5 + way)
                    gradient_out[pl.ds(first, take), cols] = value
                    return carry

                lax.fori_loop(0, pieces, step, 0)

    pl.semaphore_wait(barrier, insts - 1 + scens - 1)
    send_parts(0)
    send_parts(1)
    if number > 2:
        profit_load(2)
        profit(2, 0, blocks)
    if number > 4:
        profit_load(4)
        profit(4, 0, blocks // 2)
    sum_and_gather(0)
    if number > 2:
        send_parts(2)
    if number > 3:
        profit_load(3)
        profit(3, 0, blocks)
    if number > 4:
        profit(4, blocks // 2, blocks)
    sum_and_gather(1)
    if number > 3:
        send_parts(3)
    half = (pieces + 1) // 2
    cut = pieces // 2
    for c in range(number):
        weigh(c)
        multiply(c, 0, half)
        if c + 2 < number:
            sum_and_gather(c + 2)
        if c + 4 < number:
            send_parts(c + 4)
        if c >= 3:
            settle(c - 1)
            forward(c - 1, 0, 0, cut)
        if c >= 4:
            forward(c - 2, 1, 0, cut)
        multiply(c, half, pieces + 1)
        if c + 5 < number:
            profit_load(c + 5)
            profit(c + 5, 0, blocks)
        if c == 2:
            for n in (0, 1):
                settle(n)
                forward(n, 0, 0, pieces)
                forward(n, 1, 0, pieces)
        if c >= 4:
            forward(c - 2, 1, cut, pieces)
        if c >= 3:
            forward(c - 1, 0, cut, pieces)
    settle(number - 1)
    for c in range(number - 2):
        finish(c)

    def both(p, carry):
        if number >= 4:
            forward(number - 2, 1, p, p + 1)
        forward(number - 1, 0, p, p + 1)
        return carry

    lax.fori_loop(0, pieces, both, 0)
    forward(number - 1, 1, 0, pieces)
    finish(number - 2)
    finish(number - 1)

    share = accounts // insts
    if share % LANES == 0:
        margin_out[...] = marg[pl.ds(inst * (share // LANES), share // LANES), :]
    else:
        margin_out[...] = marg[pl.ds(inst * share // LANES, 1), :]

    for c in range(number):
        for i in range(1, insts):
            rs_copy(c, i).wait_send()
            ag_copy(c, i, inst).wait_send()
        for i in range(1, scens):
            stats_copy(c, i).wait_send()
        for slot in range(2):
            owner = owner_of(c, slot)

            def drain(p, carry):
                pair_copy(c, slot, p).wait_send()

                @pl.when(owner > z)
                def _():
                    line_copy(c, slot, p, 0).wait_send()

                @pl.when(owner < z)
                def _():
                    line_copy(c, slot, p, 1).wait_send()

                return carry

            lax.fori_loop(0, pieces, drain, 0)


def body(positions, holding_block_grid, risk):
    accounts, instruments = positions.shape
    scen_here = risk.shape[1]
    insts = lax.axis_size("inst")
    scens = lax.axis_size("scen")
    chips = scens // CORES
    rows = accounts // scens
    softness = 8.0 * math.sqrt(instruments * insts)
    plan = chunk_plan(rows, chips, insts)
    number = len(plan)
    share = accounts // insts
    most = max(4 * take for _, _, _, take in plan)
    head = 4 * (plan[0][3] + plan[1][3])
    pieces = instruments // min(PIECE, instruments)
    kblock = min(512, instruments)
    cfg = (plan, accounts, insts, scens, softness, scen_here * scens)
    dma = pltpu.SemaphoreType.DMA
    margin, gradient = pl.pallas_call(
        functools.partial(kernel, cfg),
        out_shape=(
            jax.ShapeDtypeStruct((max(1, share // LANES), LANES), jnp.float32),
            jax.ShapeDtypeStruct((rows, instruments), jnp.float32),
        ),
        in_specs=[
            pl.BlockSpec(memory_space=pl.ANY),
            pl.BlockSpec(memory_space=pltpu.SMEM),
            pl.BlockSpec(memory_space=pl.ANY),
        ],
        out_specs=(
            pl.BlockSpec(memory_space=pltpu.VMEM),
            pl.BlockSpec(memory_space=pltpu.VMEM),
        ),
        scratch_shapes=[
            pltpu.VMEM((STAGES, kblock, scen_here), jnp.float32),
            pltpu.VMEM((2, max(most, head), instruments), jnp.int32),
            pltpu.VMEM((2 * max(most, head), instruments), jnp.bfloat16),
            pltpu.VMEM((instruments, scen_here), jnp.bfloat16),
            pltpu.VMEM((instruments, scen_here), jnp.bfloat16),
            pltpu.VMEM((accounts, scen_here), jnp.float32),
            pltpu.VMEM((insts - 1, accounts // insts, scen_here), jnp.float32),
            pltpu.VMEM((accounts, scen_here), jnp.float32),
            pltpu.VMEM((2 * most, scen_here), jnp.bfloat16),
            pltpu.VMEM((LANES, LANES), jnp.float32),
            pltpu.VMEM((LANES, LANES), jnp.float32),
            pltpu.VMEM((number, scens, 2, LANES), jnp.float32),
            pltpu.VMEM((LANES, LANES), jnp.float32),
            pltpu.VMEM((number, LANES, LANES), jnp.float32),
            pltpu.VMEM((accounts, instruments), jnp.float32),
            pltpu.VMEM((accounts // 2, instruments), jnp.float32),
            pltpu.VMEM((2, accounts // 2, instruments), jnp.float32),
            pltpu.VMEM((max(8, accounts // LANES), LANES), jnp.float32),
            dma((STAGES,)),
            dma((2, 2, 4)),
            dma((number, insts - 1)),
            dma((number, insts - 1)),
            dma((number, insts - 1)),
            dma((number, insts - 1)),
            dma((number, scens - 1)),
            dma((number, scens - 1)),
            dma((number, 2, pieces)),
            dma((number, 2, pieces)),
            dma((number, 2, pieces)),
            dma((2, number, 2, pieces)),
        ],
        compiler_params=pltpu.CompilerParams(
            collective_id=0, has_side_effects=True, vmem_limit_bytes=67043328
        ),
    )(positions, holding_block_grid, risk)
    if share % LANES == 0:
        margin = margin.reshape(share)
    else:
        start = (lax.axis_index("inst") * share) % LANES
        margin = lax.dynamic_slice_in_dim(margin.reshape(LANES), start, share)
    return (margin, gradient)


def solution(mesh):
    placed = (P(None, "inst"), P(None, "inst"), P("inst", "scen"))
    return jax.shard_map(
        body, mesh=mesh, in_specs=placed, out_specs=(P("inst"), P("scen", "inst")), check_vma=False
    )
```
